256 devices in a mesh: rep: 2 (over core), dp: 128 (over x, y, z).
Axes of the slice: x: 4, y: 4, z: 8, core: 2. Of those that a mesh axis runs over, the one named last changes fastest.
Arguments:
- a: bfloat16 [256, 2, 4096, 640], P(('rep', 'dp')), parts along dimension 0
- g: bfloat16 [256, 2, 4096, 2048], P(('rep', 'dp')), parts along dimension 0
Outputs:
- output: bfloat16 [4, 640, 2048], P('rep'), parts along dimension 0
There are 2 independent parts. The reference program is written for one: setup_inputs(seed, part) draws one part's arguments, and reference() takes and returns one part's arrays. A program takes and returns all parts, laid end to end along the dimension named above; each array names one.
All inputs are finite; a program needn't handle non-finite values.
Results may differ from the reference program's by a relative error of at most 0.012.
Values are sent between devices in bfloat16 or wider.
A program may use at most 768 MiB of HBM per device.

```python
import jax
import jax.numpy as jnp
from jax import lax

DEVICES = 128
MATRICES = 2
TOKENS = 4096
D = 640
FF = 2048


def setup_inputs(seed: int = 0, part: int = 0) -> dict:
    ka, kg, ks = (jax.random.fold_in(k, part) for k in jax.random.split(jax.random.key(seed), 3))
    size = 2.0 ** jax.random.uniform(ks, (DEVICES, MATRICES, 1, 1), jnp.float32, -1.0, 1.0)
    a = jax.random.normal(ka, (DEVICES, MATRICES, TOKENS, D), jnp.float32)
    g = size * jax.random.normal(kg, (DEVICES, MATRICES, TOKENS, FF), jnp.float32) * (DEVICES * TOKENS) ** -0.5
    return {"a": a.astype(jnp.bfloat16), "g": g.astype(jnp.bfloat16)}


def reference(a, g):
    def take(so_far, one):
        term = jnp.einsum("ntd,ntf->ndf", *one, preferred_element_type=jnp.float32).astype(jnp.bfloat16)
        return so_far + term.astype(jnp.float32), None

    return lax.scan(take, jnp.zeros((MATRICES, D, FF), jnp.float32), (a, g))[0].astype(jnp.bfloat16)
```

```python
import functools

import jax
import jax.numpy as jnp
from jax import lax
from jax.experimental import pallas as pl
from jax.experimental.pallas import tpu as pltpu
from jax.sharding import PartitionSpec as P

X, Y, Z = 4, 4, 8
TOKENS, D, FF = 4096, 640, 2048
W = 1024
CW = 512
KB = 1024
SLOTS = 3
BF, F32 = jnp.bfloat16, jnp.float32

PLANS = (
    (("x", 0, 256), ("y", 256, 256), ("z", 512, 128)),
    (("x", 0, 256), ("z", 256, 256), ("y", 512, 128)),
    (("y", 0, 256), ("z", 256, 256), ("x", 512, 128)),
    (("x", 0, 256), ("y", 256, 256), ("z", 512, 128)),
)
CHUNKS = len(PLANS)
SEMS_XY, SEMS_Z = 30, 52


def scratch_of(colour, rows):
    if colour == "z":
        s = rows // Z
        return [
            pltpu.VMEM((14, s, W // 2), BF),
            pltpu.VMEM((16, s // 2, 128), BF),
            pltpu.VMEM((15, s // 2, 128), BF),
        ]
    s = rows // 4
    return [
        pltpu.VMEM((6, s // 2, W), BF),
        pltpu.VMEM((4, s // 4, W), BF),
        pltpu.VMEM((3, s // 4, W), BF),
        pltpu.VMEM((8, s // 4, 128), BF),
        pltpu.VMEM((7, s // 4, 128), BF),
    ]


class Place:
    def __init__(self):
        me = lax.axis_index("dp")
        self.first = lax.axis_index("rep") * (X * Y * Z)
        self.pos = {"x": lax.div(me, Y * Z), "y": lax.rem(lax.div(me, Z), Y), "z": lax.rem(me, Z)}
        self.spot = lax.div(me, Z)
        size = {"x": X, "y": Y, "z": Z}
        self.at = {(k, d): lax.rem(self.pos[k] + d, size[k]) if d else self.pos[k] for k in size for d in range(size[k])}
        self.plane, self.peers = {}, {}
        for dx in range(X):
            for dy in range(Y):
                self.plane[dx, dy] = self.at["x", dx] * Y + self.at["y", dy]
                self.peers[dx, dy, 0] = self.first + self.plane[dx, dy] * Z + self.pos["z"]
        for d in range(1, Z):
            self.peers[0, 0, d] = self.first + self.spot * Z + self.at["z", d]
        del self.peers[0, 0, 0]

    def peer(self, x=0, y=0, z=0):
        return self.peers[x % X, y % Y, z % Z]


class Links:
    def __init__(self, place, send_sems, recv_sems):
        self.place, self.pos, self.at = place, place.pos, place.at
        self.send_sems, self.recv_sems = send_sems, recv_sems
        self.next = 0

    def send(self, src, dst, **steps):
        i = self.next
        self.next += 1
        copy = pltpu.make_async_remote_copy(
            src_ref=src,
            dst_ref=dst,
            send_sem=self.send_sems.at[i],
            recv_sem=self.recv_sems.at[i],
            device_id=self.place.peer(**steps),
            device_id_type=pl.DeviceIdType.LOGICAL,
        )
        copy.start()
        return copy


def f32(value):
    return value.astype(F32)


def stream_xy(links, axis, other, term, out, n, col0, row0, rows, bufs):
    ra, a1, rb, a2, rc = bufs
    s, h, q = rows // 4, rows // 8, rows // 16
    p, pb, pz = links.pos[axis], links.pos[other], links.pos["z"]
    nxt, prv, far = links.at[axis, 1], links.at[axis, 3], links.at[axis, 2]
    sent = []

    def piece(j, half):
        return term.at[pl.ds(pl.multiple_of(row0 + j * s + half * h, 8), h), :]

    def go(src, dst, **steps):
        sent.append(links.send(src, dst, **steps))
        return sent[-1]

    up, down = {axis: 1}, {axis: -1}
    m0 = go(piece(far, 0), ra.at[0], **up)
    w0 = go(piece(far, 1), ra.at[3], **down)
    m1 = go(piece(nxt, 1), ra.at[1], **up)
    w1 = go(piece(prv, 0), ra.at[4], **down)
    yield
    m0.wait_recv()
    there = piece(nxt, 0)
    there[...] = (f32(there[...]) + f32(ra[0])).astype(BF)
    m2 = go(there, ra.at[2], **up)
    w0.wait_recv()
    there = piece(prv, 1)
    there[...] = (f32(there[...]) + f32(ra[3])).astype(BF)
    w2 = go(there, ra.at[5], **down)
    yield
    w1.wait_recv()
    m2.wait_recv()
    total = f32(piece(p, 0)[...]) + f32(ra[2]) + f32(ra[4])
    total = total.astype(BF)
    a1[0] = total[:q]
    a1[1] = total[q:]
    m1.wait_recv()
    w2.wait_recv()
    total = f32(piece(p, 1)[...]) + f32(ra[1]) + f32(ra[5])
    total = total.astype(BF)
    a1[2] = total[:q]
    a1[3] = total[q:]
    got = [go(a1.at[links.at[other, d]], rb.at[d - 1], **{other: d}) for d in (2, 1, 3)]
    yield
    for copy in got:
        copy.wait_recv()
    total = f32(a1[pb]) + f32(rb[0]) + f32(rb[1]) + f32(rb[2])
    total = total.astype(BF)
    for j in range(8):
        a2[j] = total[:, j * 128 : (j + 1) * 128]
    got = [go(a2.at[links.at["z", d]], rc.at[d - 1], z=d) for d in (4, 3, 5, 2, 6, 1, 7)]
    yield
    for copy in got:
        copy.wait_recv()
    total = f32(a2[pz])
    for d in range(7):
        total = total + f32(rc[d])
    row = pl.multiple_of(row0 + p * s + pb * q, 8)
    tile = out.at[n, pl.ds(row, q), pl.ds(pl.multiple_of(col0 + pz * 128, 128), 128)]
    tile[...] = total.astype(BF)
    got = [go(tile, tile, z=d) for d in (4, 3, 5, 2, 6, 1, 7)]
    yield
    for copy in got:
        copy.wait_recv()
    cols = pl.ds(col0, W)
    block = out.at[n, pl.ds(row, q), cols]
    got = [go(block, block, **{other: d}) for d in (2, 1, 3)]
    yield
    for copy in got:
        copy.wait_recv()
    shard = out.at[n, pl.ds(pl.multiple_of(row0 + p * s, 8), s), cols]
    g0, g1 = go(shard, shard, **up), go(shard, shard, **down)
    yield
    g0.wait_recv()
    half = out.at[n, pl.ds(pl.multiple_of(row0 + prv * s, 8), h), cols]
    g2 = go(half, half, **up)
    g1.wait_recv()
    half = out.at[n, pl.ds(pl.multiple_of(row0 + nxt * s + h, 8), h), cols]
    g3 = go(half, half, **down)
    yield
    for copy in sent:
        copy.wait_send()
    g2.wait_recv()
    g3.wait_recv()


def stream_z(links, term, out, n, col0, row0, rows, bufs):
    rz, az, rp = bufs
    s, hc = rows // 8, W // 2
    p = links.pos["z"]
    spot = links.place.spot
    sent = []

    def piece(j, half):
        return term.at[pl.ds(pl.multiple_of(row0 + j * s, 8), s), pl.ds(half * hc, hc)]

    def go(src, dst, **steps):
        sent.append(links.send(src, dst, **steps))
        return sent[-1]

    chains = ((1, 0, 4), (-1, 1, 4), (1, 1, 3), (-1, 0, 3))
    slot, last = 0, {}
    for t in range(4):
        for way, half, length in chains:
            if t >= length:
                continue
            there = piece(links.at["z", way * (length - t) % Z], half)
            if t:
                copy, buf = last[way, half]
                copy.wait_recv()
                there[...] = (f32(there[...]) + f32(rz[buf])).astype(BF)
            last[way, half] = go(there, rz.at[slot], z=way), slot
            slot += 1
        yield
    for half in range(2):
        total = f32(piece(p, half)[...])
        for way in (1, -1):
            copy, buf = last[way, half]
            copy.wait_recv()
            total = total + f32(rz[buf])
        total = total.astype(BF)
        for c in range(4):
            for r in range(2):
                az[r * 8 + half * 4 + c] = total[r * (s // 2) : (r + 1) * (s // 2), c * 128 : (c + 1) * 128]
    steps = sorted(((dx, dy) for dx in range(X) for dy in range(Y) if dx or dy), key=lambda v: -min(v[0], X - v[0]) - min(v[1], Y - v[1]))
    got = []
    for i, (dx, dy) in enumerate(steps):
        got.append(go(az.at[links.place.plane[dx, dy]], rp.at[i], x=dx, y=dy))
    yield
    for copy in got:
        copy.wait_recv()
    total = f32(az[spot])
    for i in range(15):
        total = total + f32(rp[i])
    row = pl.multiple_of(row0 + p * s + lax.div(spot, 8) * (s // 2), 8)
    col = pl.multiple_of(col0 + lax.rem(spot, 8) * 128, 128)
    tile = out.at[n, pl.ds(row, s // 2), pl.ds(col, 128)]
    tile[...] = total.astype(BF)
    got = [go(tile, tile, x=dx, y=dy) for dx, dy in steps]
    yield
    for copy in got:
        copy.wait_recv()

    def shard(j, half=None):
        r = pl.ds(pl.multiple_of(row0 + j * s, 8), s)
        return out.at[n, r, pl.ds(col0, W) if half is None else pl.ds(col0 + half * hc, hc)]

    mine = shard(p)
    g0, g1 = go(mine, mine, z=1), go(mine, mine, z=-1)
    yield
    for t in (1, 2, 3):
        g0.wait_recv()
        there = shard(links.at["z", Z - t], 0 if t == 3 else None)
        h0 = go(there, there, z=1)
        g1.wait_recv()
        there = shard(links.at["z", t], 1 if t == 3 else None)
        h1 = go(there, there, z=-1)
        g0, g1 = h0, h1
        yield
    for copy in sent:
        copy.wait_send()
    g0.wait_recv()
    g1.wait_recv()


def kernel(compute, comm, a_hbm, g_hbm, out, av, gv, at, acc, term, a_sem, g_sem, *rest):
    bufs, sems = rest[: -2 * 3 * CHUNKS], rest[-2 * 3 * CHUNKS :]
    blocks, per, steps = 2 * FF // CW, FF // CW, TOKENS // KB

    def a_copy(n, k):
        rows = pl.ds(k * KB, KB)
        return pltpu.make_async_copy(a_hbm.at[0, n, rows], av.at[n, rows], a_sem.at[n, k])

    def g_copy(b, k):
        rows = pl.ds(k * KB, KB)
        src = g_hbm.at[0, b // per, rows, pl.ds((b % per) * CW, CW)]
        return pltpu.make_async_copy(src, gv.at[b % SLOTS, rows], g_sem.at[b % SLOTS, k])

    if comm:
        barrier = pltpu.get_barrier_semaphore()
        place = Place()
        for peer in place.peers.values():
            pl.semaphore_signal(barrier, inc=1, device_id=peer, device_id_type=pl.DeviceIdType.LOGICAL)
    if compute:
        for k in range(steps):
            a_copy(0, k).start()
            g_copy(0, k).start()
        for b in range(1, SLOTS):
            for k in range(steps):
                g_copy(b, k).start()
        for k in range(steps):
            a_copy(1, k).start()

    active = []

    def tick():
        for stream in list(active):
            if next(stream, "end") == "end":
                active.remove(stream)

    for b in range(blocks):
        n = b // per
        c = b * CW // W
        off = (b * CW) % W
        if compute:
            for k in range(steps):
                rows = pl.ds(k * KB, KB)
                if b % per == 0:
                    a_copy(n, k).wait()
                    at[:, rows] = av[n, rows, :].T
                g_copy(b, k).wait()
                part = jnp.dot(at[:, rows], gv[b % SLOTS, rows, :], preferred_element_type=F32)
                if k == 0:
                    acc[...] = part
                elif k < steps - 1:
                    acc[...] += part
                else:
                    term[c, :, off : off + CW] = (acc[...] + part).astype(BF)
            if b + SLOTS < blocks:
                for k in range(steps):
                    g_copy(b + SLOTS, k).start()
        if not comm:
            continue
        if b == W // CW - 1:
            pl.semaphore_wait(barrier, len(place.peers))
        tick()
        if off + CW == W:
            for i, (colour, row0, rows_of) in enumerate(PLANS[c]):
                s = 2 * (3 * c + i)
                links = Links(place, sems[s], sems[s + 1])
                count = 3 if colour == "z" else 5
                mine, bufs = bufs[:count], bufs[count:]
                col0 = (c * W) % FF
                where = (term.at[c], out, c * W // FF, col0, row0, rows_of, mine)
                if colour == "z":
                    stream = stream_z(links, *where)
                else:
                    stream = stream_xy(links, colour, "y" if colour == "x" else "x", *where)
                next(stream)
                active.append(stream)
    while active:
        tick()


def call(a, g, compute=True, comm=True):
    buffers, sems = [], []
    for plan in PLANS:
        for colour, _, rows in plan:
            buffers += scratch_of(colour, rows)
            sems += [pltpu.SemaphoreType.DMA((SEMS_Z if colour == "z" else SEMS_XY,))] * 2
    steps = TOKENS // KB
    return pl.pallas_call(
        functools.partial(kernel, compute, comm),
        out_shape=jax.ShapeDtypeStruct((2, D, FF), BF),
        in_specs=[pl.BlockSpec(memory_space=pl.ANY)] * 2,
        out_specs=pl.BlockSpec(memory_space=pltpu.VMEM),
        scratch_shapes=[
            pltpu.VMEM((2, TOKENS, D), BF),
            pltpu.VMEM((SLOTS, TOKENS, CW), BF),
            pltpu.VMEM((D, TOKENS), BF),
            pltpu.VMEM((D, CW), F32),
            pltpu.VMEM((CHUNKS, D, W), BF),
            pltpu.SemaphoreType.DMA((2, steps)),
            pltpu.SemaphoreType.DMA((SLOTS, steps)),
            *buffers,
            *sems,
        ],
        compiler_params=pltpu.CompilerParams(
            collective_id=0 if comm else None, has_side_effects=True, vmem_limit_bytes=60 * 1024 * 1024
        ),
        name="grad_sums",
    )(a, g)


def solution(mesh):
    def step(a, g):
        spec = P(("rep", "dp"))
        return jax.shard_map(call, mesh=mesh, in_specs=(spec, spec), out_specs=P("rep"), check_vma=False)(a, g)

    return step
```
